32 devices in a mesh: gx: 2 (over y), gy: 4 (over z), gz: 4 (over x, core).
Axes of the slice: x: 2, y: 2, z: 4, core: 2. Of those that a mesh axis runs over, the one named last changes fastest.
Arguments:
- node_latent: bfloat16 [2, 4, 4, 512, 128], P('gx', 'gy', 'gz'), may hold values from -6 to 6
- ghost_latent: bfloat16 [2, 4, 4, 6, 64, 128], P('gx', 'gy', 'gz'), may hold values from -6 to 6
- edge_latent: bfloat16 [2, 4, 4, 2816, 128], P('gx', 'gy', 'gz'), may hold values from -6 to 6
- senders: int32 [2, 4, 4, 2816], P('gx', 'gy', 'gz'), may hold values from 0 to 895
- receivers: int32 [2, 4, 4, 2816], P('gx', 'gy', 'gz'), may hold values from 0 to 511, never falling along the last dimension, each value on 1 to 12 neighbouring positions
- export_rows: int32 [2, 4, 4, 6, 64], P('gx', 'gy', 'gz'), may hold values from 0 to 512, as said below
- node_cotangent: bfloat16 [2, 4, 4, 512, 128], P('gx', 'gy', 'gz'), may hold values from -6 to 6
- edge_cotangent: bfloat16 [2, 4, 4, 2816, 128], P('gx', 'gy', 'gz'), may hold values from -6 to 6
- w_edge_in: bfloat16 [384, 128], replicated, may hold values from -0.3125 to 0.3125
- w_edge_hidden: bfloat16 [2, 128, 128], replicated, may hold values from -0.5 to 0.5
- b_edge: float32 [3, 128], replicated, may hold values from -3 to 3
- gain_edge: float32 [128], replicated, may hold values from 0.1 to 1.9
- shift_edge: float32 [128], replicated, may hold values from -3 to 3
- w_node_in: bfloat16 [256, 128], replicated, may hold values from -0.375 to 0.375
- w_node_hidden: bfloat16 [2, 128, 128], replicated, may hold values from -0.5 to 0.5
- b_node: float32 [3, 128], replicated, may hold values from -3 to 3
- gain_node: float32 [128], replicated, may hold values from 0.1 to 1.9
Outputs:
- node_grad: float32 [2, 4, 4, 512, 128], P('gx', 'gy', 'gz')
- edge_grad: bfloat16 [2, 4, 4, 2816, 128], P('gx', 'gy', 'gz')
- grad_w_edge_in: float32 [384, 128], replicated
- grad_w_edge_hidden: float32 [2, 128, 128], replicated
- grad_b_edge: float32 [3, 128], replicated
- grad_gain_edge: float32 [128], replicated
- grad_shift_edge: float32 [128], replicated
- grad_w_node_in: float32 [256, 128], replicated
- grad_w_node_hidden: float32 [2, 128, 128], replicated
- grad_b_node: float32 [3, 128], replicated
- grad_gain_node: float32 [128], replicated
The draws below stay inside these ranges and needn't reach their ends.
Inputs may be any that keep to these rules, and one draw needn't show every extreme that they name: `export_rows`: for each block and face the leading slots hold distinct owned rows of that block; the remaining slots hold 512, marking an empty slot.
All inputs are finite; a program needn't handle non-finite values.
Results may differ from the reference program's by a relative error of at most 0.02.
Values sent between devices are 32-bit elements; how exact they have to be, the bound alone decides.
A program may use at most 64 MiB of HBM per device.

```python
import math
import jax
import jax.numpy as jnp
import numpy as np
from jax import lax

D = 128
NODES_PER_BLOCK = 512
GHOST_SLOTS = 64
EDGE_DEV = 2816
NODES = 16384
EDGES = 90112
N_GX = 2
N_GY = 4
N_GZ = 4


def draw_export_rows(key, part):
    slab_count = N_GX * N_GY * N_GZ * 6
    slab_keys = jax.random.split(jax.random.fold_in(key, 11), slab_count)

    def one_slab(slab_key):
        order_key, vacant_random_key = jax.random.split(slab_key)
        picked_slots = jax.random.permutation(order_key, NODES_PER_BLOCK)[:GHOST_SLOTS].astype(jnp.int32)
        vacant_slots = jax.random.randint(vacant_random_key, (), 0, GHOST_SLOTS // 4 + 1, dtype=jnp.int32)
        ghost_positions = jnp.arange(GHOST_SLOTS, dtype=jnp.int32)
        return jnp.where(ghost_positions < GHOST_SLOTS - vacant_slots, picked_slots, NODES_PER_BLOCK).astype(jnp.int32)
    return jax.vmap(one_slab)(slab_keys).reshape(N_GX, N_GY, N_GZ, 6, GHOST_SLOTS)


def set_ends(values, rng, low, top_value):
    longest = values.shape.index(max(values.shape))
    spots = []
    for shift in (0, 1):
        where = [jax.random.randint(jax.random.fold_in(rng, axis), (), 0, length) for axis, length in enumerate(values.shape)]
        where[longest] = (where[longest] + shift) % values.shape[longest]
        spots.append(tuple(where))
    return values.at[spots[0]].set(low).at[spots[1]].set(top_value)


def shard_levels(own_key, extent, cuts, low, largest):
    level = 1.0
    for dim, shards_of in cuts:
        draws = jax.random.uniform(jax.random.fold_in(jax.random.fold_in(own_key, 6), dim), (shards_of,), jnp.float32, low / len(cuts), largest / len(cuts))
        level = level * jnp.repeat(jnp.exp(draws), extent[dim] // shards_of).reshape((-1,) + (1,) * (len(extent) - 1 - dim))
    return level


def split_up(amount, total, limit, slope):
    portions = [(1 << 20) // math.isqrt(standing ** slope) + 1 for standing in range(2, amount + 1)]
    rest, counts = total - limit - (amount - 1), [1] * (amount - 1)
    while rest > 0:
        free = [i for i in range(amount - 1) if counts[i] < limit]
        whole, remaining = sum([portions[i] for i in free]), rest
        for i in free:
            addition = min(limit - counts[i], max(1, remaining * portions[i] // whole), rest)
            counts[i] = counts[i] + addition
            rest = rest - addition
    return np.array([limit] + counts)


def uneven_parts(stream_key, count, total, most, skew):
    if count == 2:
        one = jax.random.randint(stream_key, (), max(1, total - most), min(most, total - 1) + 1)
        return jnp.stack([one, total - one])
    lengths = jnp.asarray(split_up(count, total, most, skew), jnp.int32)
    pairs = (count - 1) // 2
    source_of, receiver = lengths[1:1 + 2 * pairs:2], lengths[2:2 + 2 * pairs:2]
    slack = jnp.minimum(source_of - 1, most - receiver)
    passed = jax.random.randint(jax.random.fold_in(stream_key, 1), (pairs,), 0, 1 << 20) % (slack + 1)
    lengths = lengths.at[1:1 + 2 * pairs:2].set(source_of - passed).at[2:2 + 2 * pairs:2].set(receiver + passed)
    return lengths[jax.random.permutation(jax.random.fold_in(stream_key, 2), count)]


def gaussian(key, dims, scale, bound, cuts=(), kind=jnp.bfloat16):
    result = jax.random.normal(key, dims, jnp.float32) * scale
    if len(cuts) > 0:
        result = shard_levels(key, dims, cuts, -0.22, 0.18) * result
    return jnp.clip(result, min=-bound, max=bound).astype(kind)


def setup_inputs(seed: int = 0) -> dict:
    key_of = jax.random.split(jax.random.key(seed), 18)
    node_latent = gaussian(key_of[0], (N_GX, N_GY, N_GZ, NODES_PER_BLOCK, D), 1.0, 6.0, ((0, 2), (1, 4), (2, 4)))
    ghost_latent = gaussian(key_of[1], (N_GX, N_GY, N_GZ, 6, GHOST_SLOTS, D), 1.0, 6.0, ((0, 2), (1, 4), (2, 4)))
    edge_latent = gaussian(key_of[2], (N_GX, N_GY, N_GZ, EDGE_DEV, D), 1.0, 6.0, ((0, 2), (1, 4), (2, 4)))
    senders = set_ends(jax.random.randint(key_of[3], (N_GX, N_GY, N_GZ, EDGE_DEV), 0, NODES_PER_BLOCK + 6 * GHOST_SLOTS), jax.random.fold_in(key_of[3], 1), 0, (NODES_PER_BLOCK + 6 * GHOST_SLOTS) - 1).astype(jnp.int32)
    receivers = jax.vmap(lambda own: jnp.searchsorted(jnp.cumsum(uneven_parts(own, NODES_PER_BLOCK, EDGE_DEV, 12, 1)), jnp.arange(EDGE_DEV), side="right"))(jax.random.split(key_of[4], N_GX * N_GY * N_GZ)).reshape((N_GX, N_GY, N_GZ, EDGE_DEV)).astype(jnp.int32)
    export_rows = draw_export_rows(jax.random.fold_in(key_of[17], 71), 0)
    node_cotangent = gaussian(key_of[6], (N_GX, N_GY, N_GZ, NODES_PER_BLOCK, D), 1.0, 6.0, ((0, 2), (1, 4), (2, 4)))
    edge_cotangent = gaussian(key_of[7], (N_GX, N_GY, N_GZ, EDGE_DEV, D), 1.0, 6.0, ((0, 2), (1, 4), (2, 4)))
    w_edge_in = gaussian(key_of[8], (3 * D, D), (3 * D) ** -0.5, 0.3125)
    w_edge_hidden = gaussian(key_of[9], (2, D, D), D ** -0.5, 0.5)
    b_edge = gaussian(key_of[10], (3, D), 0.5, 3.0, (), jnp.float32)
    gain_edge = jnp.clip(1.0 + 0.18 * jax.random.normal(key_of[11], (D,), jnp.float32), 0.1, 1.9)
    shift_edge = gaussian(key_of[12], (D,), 0.5, 3.0, (), jnp.float32)
    w_node_in = gaussian(key_of[13], (2 * D, D), (2 * D) ** -0.5, 0.375)
    w_node_hidden = gaussian(key_of[14], (2, D, D), D ** -0.5, 0.5)
    b_node = gaussian(key_of[15], (3, D), 0.5, 3.0, (), jnp.float32)
    gain_node = jnp.clip(1.0 + 0.18 * jax.random.normal(key_of[16], (D,), jnp.float32), 0.1, 1.9)
    return dict(node_latent=node_latent, ghost_latent=ghost_latent, edge_latent=edge_latent, senders=senders, receivers=receivers, export_rows=export_rows, node_cotangent=node_cotangent, edge_cotangent=edge_cotangent, w_edge_in=w_edge_in, w_edge_hidden=w_edge_hidden, b_edge=b_edge, gain_edge=gain_edge, shift_edge=shift_edge, w_node_in=w_node_in, w_node_hidden=w_node_hidden, b_node=b_node, gain_node=gain_node)


EPSILON = 1e-05

def matmul(left, right):
    return jnp.dot(left, right, preferred_element_type=jnp.float32)

def contract_rows(left, right):
    return lax.dot_general(left, right, (((0,), (0,)), ((), ())), preferred_element_type=jnp.float32)

def silu_parts(preact):
    sigmoid = jax.nn.sigmoid(preact)
    return (preact * sigmoid, sigmoid * (1.0 + preact * (1.0 - sigmoid)))

def norm_parts(preact):
    centred = preact - lax.optimization_barrier(jnp.mean(preact, -1, keepdims=True))
    inv_std = lax.rsqrt(lax.optimization_barrier(jnp.mean(centred * centred, -1, keepdims=True)) + EPSILON)
    return (centred * inv_std, inv_std)

def norm_back(grad_out, gain, normed, inv_std):
    scaled = grad_out * gain
    return inv_std * (scaled - lax.optimization_barrier(jnp.mean(scaled, -1, keepdims=True)) - normed * lax.optimization_barrier(jnp.mean(scaled * normed, -1, keepdims=True)))

def mlp_forward(inputs, w_first, w_hidden, biases):
    first_pre = matmul(inputs, w_first) + biases[0]
    first_act, first_slope = silu_parts(first_pre)
    first_out = first_act.astype(jnp.bfloat16)
    second_pre = matmul(first_out, w_hidden[0]) + biases[1]
    second_act, second_slope = silu_parts(second_pre)
    second_out = second_act.astype(jnp.bfloat16)
    final_pre = matmul(second_out, w_hidden[1]) + biases[2]
    return ((first_out, second_out, first_slope, second_slope), final_pre)

def mlp_back_inputs(final_grad, saved, w_first, w_hidden):
    first_out, second_out, first_slope, second_slope = saved
    final_round = final_grad.astype(jnp.bfloat16)
    second_grad = matmul(final_round, w_hidden[1].T) * second_slope
    second_round = second_grad.astype(jnp.bfloat16)
    first_grad = matmul(second_round, w_hidden[0].T) * first_slope
    first_round = first_grad.astype(jnp.bfloat16)
    input_grad = matmul(first_round, w_first.T)
    bias_grad = jnp.stack([lax.optimization_barrier(jnp.sum(first_grad, 0)), lax.optimization_barrier(jnp.sum(second_grad, 0)), lax.optimization_barrier(jnp.sum(final_grad, 0))])
    return ((first_round, second_round, final_round), bias_grad, input_grad)

def mlp_back_weights(inputs, saved, rounded):
    first_weight = contract_rows(inputs, rounded[0])
    hidden_weight = jnp.stack([contract_rows(saved[0], rounded[1]), contract_rows(saved[1], rounded[2])])
    return (first_weight, hidden_weight)

def forward_states(node_rows, ghost_rows, edge_rows, sender_ids, receiver_ids, params):
    node_count, feature_width = node_rows.shape
    full_rows = jnp.concatenate([node_rows, ghost_rows.reshape(-1, feature_width)], 0)
    edge_inputs = jnp.concatenate([edge_rows, full_rows[sender_ids], full_rows[receiver_ids]], 1)
    edge_stored_state, edge_pre = mlp_forward(edge_inputs, params[0], params[1], params[2])
    edge_normed, edge_inv = norm_parts(edge_pre)
    edge_new = (edge_normed * params[3] + params[4]).astype(jnp.bfloat16)
    aggregate = jax.ops.segment_sum(edge_new.astype(jnp.float32), receiver_ids, num_segments=node_count).astype(jnp.bfloat16)
    node_input_rows = jnp.concatenate([node_rows, aggregate], 1)
    node_saved, node_pre = mlp_forward(node_input_rows, params[5], params[6], params[7])
    node_normed, node_inv = norm_parts(node_pre)
    return ((edge_inputs, edge_stored_state, edge_normed, edge_inv), (node_input_rows, node_saved, node_normed, node_inv))

def node_backward(node_state, node_cot, params):
    node_input_rows, node_saved, node_normed, node_inv = node_state
    upstream = node_cot.astype(jnp.float32)
    gain_grad = lax.optimization_barrier(jnp.sum(upstream * node_normed, 0))
    final_grad = norm_back(upstream, params[8], node_normed, node_inv)
    rounded, bias_grad, input_grad = mlp_back_inputs(final_grad, node_saved, params[5], params[6])
    first_weight, hidden_weight = mlp_back_weights(node_input_rows, node_saved, rounded)
    return (input_grad, (first_weight, hidden_weight, bias_grad, gain_grad))

def edge_backward_inputs(edge_state, edge_cot, agg_grad, sender_ids, receiver_ids, total_rows, params):
    edge_inputs, edge_stored_state, edge_normed, edge_inv = edge_state
    feature_width = edge_cot.shape[1]
    edge_upstream = edge_cot.astype(jnp.float32)
    new_grad = edge_upstream + agg_grad[receiver_ids]
    gain_grad = lax.optimization_barrier(jnp.sum(new_grad * edge_normed, 0))
    shift_grad = lax.optimization_barrier(jnp.sum(new_grad, 0))
    final_grad = norm_back(new_grad, params[3], edge_normed, edge_inv)
    rounded, bias_grad, input_grad = mlp_back_inputs(final_grad, edge_stored_state, params[0], params[1])
    edge_grad = (edge_upstream + input_grad[:, :feature_width]).astype(jnp.bfloat16)
    full_grad = jax.ops.segment_sum(input_grad[:, feature_width:2 * feature_width], sender_ids, num_segments=total_rows)
    full_grad = full_grad + jax.ops.segment_sum(input_grad[:, 2 * feature_width:], receiver_ids, num_segments=total_rows)
    return (edge_grad, full_grad, rounded, (bias_grad, gain_grad, shift_grad))

def block_pass(node_rows, ghost_rows, edge_rows, sender_ids, receiver_ids, node_cot, edge_cot, params):
    node_count, feature_width = node_rows.shape
    total_rows = node_count + ghost_rows.shape[0] * ghost_rows.shape[1]
    edge_state, node_state = forward_states(node_rows, ghost_rows, edge_rows, sender_ids, receiver_ids, params)
    node_input_grad, node_weights = node_backward(node_state, node_cot, params)
    edge_grad, full_grad, rounded, edge_small = edge_backward_inputs(edge_state, edge_cot, node_input_grad[:, feature_width:], sender_ids, receiver_ids, total_rows, params)
    first_weight, hidden_weight = mlp_back_weights(edge_state[0], edge_state[1], rounded)
    local_grad = node_cot.astype(jnp.float32) + node_input_grad[:, :feature_width] + full_grad[:node_count]
    ghost_grad = full_grad[node_count:].reshape(ghost_rows.shape)
    weights = (first_weight, hidden_weight) + edge_small + node_weights
    return (local_grad, ghost_grad, edge_grad, weights)

def add_rows(target, rows, values):
    return target.at[rows].add(values, mode='drop')

def reference(node_latent, ghost_latent, edge_latent, senders, receivers, export_rows, node_cotangent, edge_cotangent, w_edge_in, w_edge_hidden, b_edge, gain_edge, shift_edge, w_node_in, w_node_hidden, b_node, gain_node):
    params = (w_edge_in, w_edge_hidden, b_edge, gain_edge, shift_edge, w_node_in, w_node_hidden, b_node, gain_node)
    block_count = N_GX * N_GY * N_GZ
    grid_shape = (N_GX, N_GY, N_GZ)

    def flatten(array):
        return array.reshape((block_count,) + array.shape[3:])
    stacked = tuple((flatten(array) for array in (node_latent, ghost_latent, edge_latent, senders, receivers, node_cotangent, edge_cotangent)))

    def visit(running, block_item):
        local_grad, ghost_grad, edge_grad, weights = block_pass(*block_item, params)
        return (tuple((total + term for total, term in zip(running, weights))), (local_grad, ghost_grad, edge_grad))
    start = tuple((jnp.zeros(param.shape, jnp.float32) for param in params))
    totals, (local_all, ghost_all, edge_all) = lax.scan(visit, start, stacked)
    ghost_grid = ghost_all.reshape(grid_shape + ghost_all.shape[1:])
    rows_flat = flatten(export_rows)
    node_grad = local_all
    for face_index in range(6):
        incoming = jnp.roll(ghost_grid[:, :, :, face_index], 1 - 2 * (face_index % 2), face_index // 2)
        node_grad = jax.vmap(add_rows)(node_grad, rows_flat[:, face_index], flatten(incoming))
    node_grad = node_grad.reshape(grid_shape + node_grad.shape[1:])
    edge_grad = edge_all.reshape(grid_shape + edge_all.shape[1:])
    edge_scale = EDGES ** (-0.5)
    node_scale = NODES ** (-0.5)
    return (node_grad, edge_grad, totals[0] * edge_scale, totals[1] * edge_scale, totals[2] * edge_scale, totals[3] * edge_scale, totals[4] * edge_scale, totals[5] * node_scale, totals[6] * node_scale, totals[7] * node_scale, totals[8] * node_scale)
```

```python
import functools

import jax
import jax.numpy as jnp
from jax import lax
from jax.experimental import pallas as pl
from jax.experimental.pallas import tpu as pltpu
from jax.sharding import PartitionSpec as P

EPSILON = 1e-05
LANES = 128
EDGE_TILES = 2
MESH = pl.DeviceIdType.MESH
AXES = ("gx", "gy", "gz")


def matmul(left, right):
    return jnp.dot(left, right, preferred_element_type=jnp.float32)


def matmul_nt(left, right):
    return lax.dot_general(
        left, right, (((1,), (1,)), ((), ())), preferred_element_type=jnp.float32
    )


def contract_rows(left, right):
    return lax.dot_general(
        left, right, (((0,), (0,)), ((), ())), preferred_element_type=jnp.float32
    )


def silu_parts(preact):
    sigmoid = 0.5 * jnp.tanh(0.5 * preact) + 0.5
    act = preact * sigmoid
    return act, sigmoid + act * (1.0 - sigmoid)


def norm_parts(preact):
    centred = preact - jnp.mean(preact, -1, keepdims=True)
    inv_std = lax.rsqrt(jnp.mean(centred * centred, -1, keepdims=True) + EPSILON)
    return centred * inv_std, inv_std


def norm_back(grad_out, gain, normed, inv_std):
    scaled = grad_out * gain
    return inv_std * (
        scaled
        - jnp.mean(scaled, -1, keepdims=True)
        - normed * jnp.mean(scaled * normed, -1, keepdims=True)
    )


def rows_sum(values):
    return jnp.sum(values, 0, keepdims=True)


def one_hot(hit):
    return jnp.where(hit, 1.0, 0.0).astype(jnp.bfloat16)


def compute_kernel(
    edge_scale,
    node_scale,
    node,
    ghost,
    edge,
    snd,
    rcv,
    ncot,
    ecot,
    we1,
    weh,
    be,
    ge,
    se,
    wn1,
    wnh,
    bn,
    gn,
    local_o,
    ghost_o,
    edge_o,
    pack_o,
    pick,
    put,
    table,
    z1_s,
    z2_s,
    slope1_s,
    slope2_s,
    normed_s,
    inv_s,
    agg_s,
    acc,
    wacc,
    small,
):
    nodes, width = node.shape
    edges = edge.shape[0]
    ghosts = ghost.shape[0]
    total = nodes + ghosts
    bf16 = jnp.bfloat16
    tile = edges // EDGE_TILES

    lane = lax.broadcasted_iota(jnp.int32, (LANES, LANES), 1)
    sub = lax.broadcasted_iota(jnp.int32, (LANES, LANES), 0)

    def build(block, carry):
        at = pl.ds(pl.multiple_of(block * LANES, LANES), LANES)
        for ids, base, count in ((snd, 0, total), (rcv, total, nodes)):
            row = jnp.broadcast_to(ids[:, at], (LANES, LANES))
            column = jnp.transpose(row)
            for part in range(count // LANES):
                where = base + part * LANES
                pick[at, where : where + LANES] = one_hot(column == lane + part * LANES)
                put[where : where + LANES, at] = one_hot(row == sub + part * LANES)
        return carry

    lax.fori_loop(0, edges // LANES, build, 0)

    table[:nodes] = matmul(node[...], we1[width : 2 * width]).astype(bf16)
    table[nodes:total] = matmul(ghost[...], we1[width : 2 * width]).astype(bf16)
    table[total:] = matmul(node[...], we1[2 * width :]).astype(bf16)
    agg_s[...] = jnp.zeros_like(agg_s)
    acc[...] = jnp.zeros_like(acc)
    wacc[...] = jnp.zeros_like(wacc)
    small[...] = jnp.zeros_like(small)

    def forward(step, carry):
        at = pl.ds(pl.multiple_of(step * tile, LANES), tile)
        first = matmul(edge[at], we1[:width]) + matmul(pick[at], table[...]) + be[0:1]
        act, slope = silu_parts(first)
        z1 = act.astype(bf16)
        z1_s[at] = z1
        slope1_s[at] = slope
        act, slope = silu_parts(matmul(z1, weh[0]) + be[1:2])
        z2 = act.astype(bf16)
        z2_s[at] = z2
        slope2_s[at] = slope
        normed, inv = norm_parts(matmul(z2, weh[1]) + be[2:3])
        normed_s[at] = normed
        inv_s[at] = jnp.broadcast_to(inv, normed.shape)
        new = (normed * ge[...] + se[...]).astype(bf16)
        agg_s[...] += matmul(put[total:, at], new)
        return carry

    lax.fori_loop(0, EDGE_TILES, forward, 0)

    agg = agg_s[...].astype(bf16)
    first = matmul(node[...], wn1[:width]) + matmul(agg, wn1[width:]) + bn[0:1]
    act, slope1 = silu_parts(first)
    z1 = act.astype(bf16)
    act, slope2 = silu_parts(matmul(z1, wnh[0]) + bn[1:2])
    z2 = act.astype(bf16)
    normed, inv = norm_parts(matmul(z2, wnh[1]) + bn[2:3])
    up = ncot[...].astype(jnp.float32)
    gain_row = rows_sum(up * normed)
    g3 = norm_back(up, gn[...], normed, inv)
    r3 = g3.astype(bf16)
    g2 = matmul_nt(r3, wnh[1]) * slope2
    r2 = g2.astype(bf16)
    g1 = matmul_nt(r2, wnh[0]) * slope1
    r1 = g1.astype(bf16)
    local_o[...] = up + matmul_nt(r1, wn1[:width])
    agg_grad = matmul_nt(r1, wn1[width:]).astype(bf16)
    base = 5 * width
    pack_o[base : base + width] = contract_rows(node[...], r1) * node_scale
    pack_o[base + width : base + 2 * width] = contract_rows(agg, r1) * node_scale
    pack_o[base + 2 * width : base + 3 * width] = contract_rows(z1, r2) * node_scale
    pack_o[base + 3 * width : base + 4 * width] = contract_rows(z2, r3) * node_scale
    tail = 9 * width
    pack_o[tail:] = jnp.zeros((pack_o.shape[0] - tail, width), jnp.float32)
    for index, row in enumerate((rows_sum(g1), rows_sum(g2), rows_sum(g3), gain_row)):
        spot = tail + 5 + index
        pack_o[spot : spot + 1] = row * node_scale

    def backward(step, carry):
        at = pl.ds(pl.multiple_of(step * tile, LANES), tile)
        cot = ecot[at].astype(jnp.float32)
        up = cot + matmul(pick[at, total:], agg_grad)
        normed = normed_s[at]
        g3 = norm_back(up, ge[...], normed, inv_s[at])
        r3 = g3.astype(bf16)
        g2 = matmul_nt(r3, weh[1]) * slope2_s[at]
        r2 = g2.astype(bf16)
        g1 = matmul_nt(r2, weh[0]) * slope1_s[at]
        r1 = g1.astype(bf16)
        edge_o[at] = (cot + matmul_nt(r1, we1[:width])).astype(bf16)
        acc[...] += matmul(put[:, at], r1)
        wacc[:width] += contract_rows(edge[at], r1)
        wacc[width : 2 * width] += contract_rows(z1_s[at], r2)
        wacc[2 * width :] += contract_rows(z2_s[at], r3)
        for index, term in enumerate((g1, g2, g3, up * normed, up)):
            small[index : index + 1] += rows_sum(term)
        return carry

    lax.fori_loop(0, EDGE_TILES, backward, 0)

    by_sender = acc[:total].astype(bf16)
    by_receiver = acc[total:].astype(bf16)
    full = matmul_nt(by_sender, we1[width : 2 * width])
    local_o[...] += full[:nodes] + matmul_nt(by_receiver, we1[2 * width :])
    ghost_o[...] = full[nodes:]
    pack_o[:width] = wacc[:width] * edge_scale
    middle = contract_rows(node[...], by_sender[:nodes])
    middle += contract_rows(ghost[...], by_sender[nodes:])
    pack_o[width : 2 * width] = middle * edge_scale
    pack_o[2 * width : 3 * width] = contract_rows(node[...], by_receiver) * edge_scale
    pack_o[3 * width : 5 * width] = wacc[width:] * edge_scale
    pack_o[tail : tail + 5] = small[:5] * edge_scale


def stages_of(sizes):
    stages = [("gz", 2, 1), ("gz", sizes["gz"] // 2, 2), ("gx", sizes["gx"], 1)]
    stages.append(("gy", sizes["gy"], 1))
    return [stage for stage in stages if stage[1] > 1]


def member(stage):
    axis, count, stride = stage
    return lax.rem(lax.axis_index(axis) // stride, count)


def peer(stage, distance):
    axis, count, stride = stage
    mine = member(stage)
    other = lax.rem(mine + distance, count)
    return other, {axis: lax.axis_index(axis) + (other - mine) * stride}


def comm_kernel(sizes, *refs):
    stages = stages_of(sizes)
    pack, ghost, out, halo = refs[:4]
    own = refs[4]
    landing = refs[5 : 5 + len(stages)]
    sums = refs[5 + len(stages) : 5 + 2 * len(stages)]
    ssem, rsem, asem, gsem, hs, hr, lsem = refs[5 + 2 * len(stages) :]

    def face_target(face):
        axis, side = AXES[face // 2], face % 2
        count = sizes[axis]
        step = 1 if side == 0 else count - 1
        return {axis: lax.rem(lax.axis_index(axis) + step, count)}

    barrier = pltpu.get_barrier_semaphore()
    greeted = 0
    for face in range(6):
        pl.semaphore_signal(barrier, inc=1, device_id=face_target(face), device_id_type=MESH)
        greeted += 1
    for stage in stages:
        for distance in range(1, stage[1]):
            pl.semaphore_signal(
                barrier, inc=1, device_id=peer(stage, distance)[1], device_id_type=MESH
            )
            greeted += 1
    pl.semaphore_wait(barrier, greeted)

    slots = ghost.shape[0] // 6
    faces = []
    for face in range(6):
        rows = pl.ds(face * slots, slots)
        copy = pltpu.make_async_remote_copy(
            src_ref=ghost.at[rows],
            dst_ref=halo.at[rows],
            send_sem=hs.at[face],
            recv_sem=hr.at[face],
            device_id=face_target(face),
            device_id_type=MESH,
        )
        faces.append(copy)

    source = pack
    length = pack.shape[0]
    offset = 0
    segments = []
    slot = 0
    for index, stage in enumerate(stages):
        count = stage[1]
        piece = length // count
        copies = []
        for distance in range(1, count):
            other, device = peer(stage, distance)
            copy = pltpu.make_async_remote_copy(
                src_ref=source.at[pl.ds(pl.multiple_of(other * piece, 8), piece)],
                dst_ref=landing[index].at[distance - 1],
                send_sem=ssem.at[slot],
                recv_sem=rsem.at[slot],
                device_id=device,
                device_id_type=MESH,
            )
            copy.start()
            copies.append(copy)
            slot += 1
        if index == 0:
            for copy in faces:
                copy.start()
        mine = member(stage)
        for copy in copies:
            copy.wait()
        summed = source[pl.ds(pl.multiple_of(mine * piece, 8), piece)]
        for distance in range(1, count):
            summed = summed + landing[index][distance - 1]
        sums[index][...] = summed
        offset = offset + mine * piece
        segments.append((stage, offset, piece))
        source = sums[index]
        length = piece

    home = pl.ds(pl.multiple_of(offset, 8), length)
    out[home] = source[...]
    slot = 0
    for stage, start, piece in reversed(segments):
        count = stage[1]
        rows = pl.ds(pl.multiple_of(start, 8), piece)
        copies = []
        for distance in range(1, count):
            device = peer(stage, distance)[1]
            copy = pltpu.make_async_remote_copy(
                src_ref=out.at[rows],
                dst_ref=out.at[rows],
                send_sem=asem.at[slot],
                recv_sem=gsem.at[slot],
                device_id=device,
                device_id_type=MESH,
            )
            copy.start()
            copies.append(copy)
            slot += 1
        for copy in copies:
            copy.wait()
    for copy in faces:
        copy.wait()


def finish_kernel(
    packed, local, halo, faces, node_o, we1_o, weh_o, be_o, ge_o, se_o, wn1_o, wnh_o, bn_o, gn_o
):
    nodes, width = local.shape
    slots = faces.shape[1]
    spot = lax.broadcasted_iota(jnp.int32, (nodes, slots), 0)
    total = local[...]
    for face in range(6):
        hit = one_hot(spot == faces[face : face + 1])
        values = halo[face * slots : (face + 1) * slots].astype(jnp.bfloat16)
        total = total + matmul(hit, values)
    node_o[...] = total
    we1_o[...] = packed[: 3 * width]
    weh_o[0] = packed[3 * width : 4 * width]
    weh_o[1] = packed[4 * width : 5 * width]
    wn1_o[...] = packed[5 * width : 7 * width]
    wnh_o[0] = packed[7 * width : 8 * width]
    wnh_o[1] = packed[8 * width : 9 * width]
    tail = 9 * width
    be_o[...] = packed[tail : tail + 3]
    ge_o[...] = packed[tail + 3 : tail + 4]
    se_o[...] = packed[tail + 4 : tail + 5]
    bn_o[...] = packed[tail + 5 : tail + 8]
    gn_o[...] = packed[tail + 8 : tail + 9]


VMEM = pl.BlockSpec(memory_space=pltpu.VMEM)


def on_device(
    sizes,
    node_latent,
    ghost_latent,
    edge_latent,
    senders,
    receivers,
    export_rows,
    node_cotangent,
    edge_cotangent,
    w_edge_in,
    w_edge_hidden,
    b_edge,
    gain_edge,
    shift_edge,
    w_node_in,
    w_node_hidden,
    b_node,
    gain_node,
):
    f32, bf16 = jnp.float32, jnp.bfloat16
    nodes, width = node_latent.shape[3:]
    slots = ghost_latent.shape[4]
    ghosts = 6 * slots
    edges = edge_latent.shape[3]
    total = nodes + ghosts
    devices = sizes["gx"] * sizes["gy"] * sizes["gz"]
    edge_scale = float(edges * devices) ** (-0.5)
    node_scale = float(nodes * devices) ** (-0.5)
    unit = 8 * devices
    packed_rows = -(-(9 * width + 9) // unit) * unit

    def shape(*dims, dtype=f32):
        return jax.ShapeDtypeStruct(dims, dtype)

    local, ghost_grad, edge_grad, packed = pl.pallas_call(
        functools.partial(compute_kernel, edge_scale, node_scale),
        out_shape=(
            shape(nodes, width),
            shape(ghosts, width),
            shape(edges, width, dtype=bf16),
            shape(packed_rows, width),
        ),
        in_specs=[VMEM] * 16,
        out_specs=(VMEM,) * 4,
        scratch_shapes=[
            pltpu.VMEM((edges, total + nodes), bf16),
            pltpu.VMEM((total + nodes, edges), bf16),
            pltpu.VMEM((total + nodes, width), bf16),
            pltpu.VMEM((edges, width), bf16),
            pltpu.VMEM((edges, width), bf16),
            pltpu.VMEM((edges, width), f32),
            pltpu.VMEM((edges, width), f32),
            pltpu.VMEM((edges, width), f32),
            pltpu.VMEM((edges, width), f32),
            pltpu.VMEM((nodes, width), f32),
            pltpu.VMEM((total + nodes, width), f32),
            pltpu.VMEM((3 * width, width), f32),
            pltpu.VMEM((8, width), f32),
        ],
        compiler_params=pltpu.CompilerParams(vmem_limit_bytes=60 * 1024 * 1024),
        name="block_pass",
    )(
        node_latent.reshape(nodes, width),
        ghost_latent.reshape(ghosts, width),
        edge_latent.reshape(edges, width),
        senders.reshape(1, edges),
        receivers.reshape(1, edges),
        node_cotangent.reshape(nodes, width),
        edge_cotangent.reshape(edges, width),
        w_edge_in,
        w_edge_hidden,
        b_edge,
        gain_edge.reshape(1, width),
        shift_edge.reshape(1, width),
        w_node_in,
        w_node_hidden,
        b_node,
        gain_node.reshape(1, width),
    )

    stages = stages_of(sizes)
    landing, sums = [], []
    length = packed_rows
    hops = 0
    for stage in stages:
        length //= stage[1]
        landing.append(pltpu.VMEM((stage[1] - 1, length, width), f32))
        sums.append(pltpu.VMEM((length, width), f32))
        hops += stage[1] - 1
    dma = pltpu.SemaphoreType.DMA
    reduced, halo = pl.pallas_call(
        functools.partial(comm_kernel, sizes),
        out_shape=(shape(packed_rows, width), shape(ghosts, width)),
        in_specs=[VMEM] * 2,
        out_specs=(VMEM,) * 2,
        scratch_shapes=[pltpu.VMEM((8, width), f32)]
        + landing
        + sums
        + [dma((hops,)), dma((hops,)), dma((hops,)), dma((hops,)), dma((6,)), dma((6,)), dma((1,))],
        compiler_params=pltpu.CompilerParams(collective_id=0, has_side_effects=True),
        name="exchange",
    )(packed, ghost_grad)

    outs = pl.pallas_call(
        finish_kernel,
        out_shape=(
            shape(nodes, width),
            shape(3 * width, width),
            shape(2, width, width),
            shape(3, width),
            shape(1, width),
            shape(1, width),
            shape(2 * width, width),
            shape(2, width, width),
            shape(3, width),
            shape(1, width),
        ),
        in_specs=[VMEM] * 4,
        out_specs=(VMEM,) * 10,
        name="finish",
    )(reduced, local, halo, export_rows.reshape(6, slots))
    node_grad, we1, weh, be, ge, se, wn1, wnh, bn, gn = outs
    return (
        node_grad.reshape(node_latent.shape),
        edge_grad.reshape(edge_latent.shape),
        we1,
        weh,
        be,
        ge.reshape(width),
        se.reshape(width),
        wn1,
        wnh,
        bn,
        gn.reshape(width),
    )


def solution(mesh):
    block = P("gx", "gy", "gz")
    sizes = dict(mesh.shape)
    return jax.shard_map(
        functools.partial(on_device, sizes),
        mesh=mesh,
        in_specs=(block,) * 8 + (P(),) * 9,
        out_specs=(block,) * 2 + (P(),) * 9,
        check_vma=False,
    )
```

```python
import functools

import jax
import jax.numpy as jnp
from jax import lax
from jax.experimental import pallas as pl
from jax.experimental.pallas import tpu as pltpu
from jax.sharding import PartitionSpec as P

EPSILON = 1e-05
LANES = 128
FORWARD_TILES = 2
BACKWARD_TILES = 4
MESH = pl.DeviceIdType.MESH
AXES = ("gx", "gy", "gz")


def matmul(left, right):
    return jnp.dot(left, right, preferred_element_type=jnp.float32)


def matmul_nt(left, right):
    return lax.dot_general(
        left, right, (((1,), (1,)), ((), ())), preferred_element_type=jnp.float32
    )


def contract_rows(left, right):
    return lax.dot_general(
        left, right, (((0,), (0,)), ((), ())), preferred_element_type=jnp.float32
    )


def silu_parts(preact):
    sigmoid = 0.5 * jnp.tanh(0.5 * preact) + 0.5
    act = preact * sigmoid
    return act, sigmoid + act * (1.0 - sigmoid)


def norm_parts(preact):
    centred = preact - jnp.mean(preact, -1, keepdims=True)
    inv_std = lax.rsqrt(jnp.mean(centred * centred, -1, keepdims=True) + EPSILON)
    return centred * inv_std, inv_std


def norm_back(grad_out, gain, normed, inv_std):
    scaled = grad_out * gain
    return inv_std * (
        scaled
        - jnp.mean(scaled, -1, keepdims=True)
        - normed * jnp.mean(scaled * normed, -1, keepdims=True)
    )


def rows_sum(values):
    return jnp.sum(values, 0, keepdims=True)


def one_hot(hit):
    return jnp.where(hit, 1.0, 0.0).astype(jnp.bfloat16)


def stage_groups(sizes):
    core = [("gz", 2, 1)]
    near = [("gx", sizes["gx"], 1), ("gz", sizes["gz"] // 2, 2)]
    far = [("gy", sizes["gy"], 1)]
    return core, near, far


def group_size(group):
    count = 1
    for _, members, _ in group:
        count *= members
    return count


def coordinate(part):
    axis, count, stride = part
    return lax.rem(lax.axis_index(axis) // stride, count)


def member(group):
    index = 0
    for part in group:
        index = index * part[1] + coordinate(part)
    return index


def peers(group):
    steps = [()]
    for part in group:
        steps = [step + (more,) for step in steps for more in range(part[1])]
    found = []
    for step in steps[1:]:
        index = 0
        device = {}
        for part, more in zip(group, step):
            axis, count, stride = part
            mine = coordinate(part)
            other = lax.rem(mine + more, count)
            index = index * count + other
            here = device.get(axis, lax.axis_index(axis))
            device[axis] = here + (other - mine) * stride
        found.append((index, device))
    return found


class Reducer:
    def __init__(self, groups, source, out, scratch):
        self.groups = groups
        self.out = out
        self.source = source
        count = len(groups)
        self.landing = scratch[:count]
        self.sums = scratch[count : 2 * count]
        self.sems = scratch[2 * count :]
        self.length = source.shape[0]
        self.offset = 0
        self.segments = []
        self.slot = 0
        self.pending = []

    def send(self, source, target, device, sends, lands):
        copy = pltpu.make_async_remote_copy(
            src_ref=source,
            dst_ref=target,
            send_sem=self.sems[sends].at[self.slot],
            recv_sem=self.sems[lands].at[self.slot],
            device_id=device,
            device_id_type=MESH,
        )
        copy.start()
        self.pending.append(copy)
        self.slot += 1

    def wait(self):
        for copy in self.pending:
            copy.wait()
        self.pending = []

    def scatter(self):
        index = len(self.segments)
        group = self.groups[index]
        piece = self.length // group_size(group)
        for spot, (other, device) in enumerate(peers(group)):
            rows = pl.ds(pl.multiple_of(other * piece, 8), piece)
            self.send(self.source.at[rows], self.landing[index].at[spot], device, 0, 1)

    def add(self):
        index = len(self.segments)
        group = self.groups[index]
        piece = self.length // group_size(group)
        self.wait()
        mine = member(group)
        total = self.source[pl.ds(pl.multiple_of(mine * piece, 8), piece)]
        for spot in range(group_size(group) - 1):
            total = total + self.landing[index][spot]
        self.offset = self.offset + mine * piece
        self.segments.append((group, self.offset, piece))
        if len(self.segments) == len(self.groups):
            self.out[pl.ds(pl.multiple_of(self.offset, 8), piece)] = total
            self.slot = 0
        else:
            self.sums[index][...] = total
            self.source = self.sums[index]
            self.length = piece

    def gather(self):
        group, start, piece = self.segments.pop()
        rows = pl.ds(pl.multiple_of(start, 8), piece)
        for _, device in peers(group):
            self.send(self.out.at[rows], self.out.at[rows], device, 2, 3)


def reducer_scratch(groups, rows, width):
    landing, sums, hops = [], [], 0
    for group in groups:
        rows //= group_size(group)
        landing.append(pltpu.VMEM((group_size(group) - 1, rows, width), jnp.float32))
        sums.append(pltpu.VMEM((rows, width), jnp.float32))
        hops += group_size(group) - 1
    return landing + sums + [pltpu.SemaphoreType.DMA((hops,))] * 4


def split_tiles(blocks, tiles):
    sizes = [blocks // tiles + (index < blocks % tiles) for index in range(tiles)]
    starts = [sum(sizes[:index]) for index in range(tiles)]
    return [(LANES * start, LANES * size) for start, size in zip(starts, sizes)]


def face_target(sizes, face):
    axis, side = AXES[face // 2], face % 2
    count = sizes[axis]
    step = 1 if side == 0 else count - 1
    return {axis: lax.rem(lax.axis_index(axis) + step, count)}


def block_kernel(
    sizes,
    edge_scale,
    node_scale,
    node,
    ghost,
    edge,
    snd,
    rcv,
    faces,
    ncot,
    ecot,
    we1,
    weh,
    be,
    ge,
    se,
    wn1,
    wnh,
    bn,
    gn,
    node_o,
    edge_o,
    nred_o,
    ared_o,
    bred_o,
    pick,
    put,
    table,
    z1_s,
    z2_s,
    r1_s,
    slope1_s,
    slope2_s,
    normed_s,
    inv_s,
    npack,
    apack,
    bpack,
    ghost_s,
    halo,
    hsend,
    hland,
    *scratch,
):
    nodes, width = node.shape
    edges = edge.shape[0]
    ghosts = ghost.shape[0]
    slots = ghosts // 6
    total = nodes + ghosts
    bf16, f32 = jnp.bfloat16, jnp.float32
    core, near, far = stage_groups(sizes)
    third = len(scratch) // 3
    node_red = Reducer([core, near, far], npack, nred_o, scratch[:third])
    a_red = Reducer([core, near, far], apack, ared_o, scratch[third : 2 * third])
    b_red = Reducer([core, far, near], bpack, bred_o, scratch[2 * third :])

    barrier = pltpu.get_barrier_semaphore()
    greeted = [face_target(sizes, face) for face in range(6)]
    for group in (core, near, far):
        greeted += [device for _, device in peers(group)]
    for device in greeted:
        pl.semaphore_signal(barrier, inc=1, device_id=device, device_id_type=MESH)

    lane = lax.broadcasted_iota(jnp.int32, (LANES, LANES), 1)
    sub = lax.broadcasted_iota(jnp.int32, (LANES, LANES), 0)

    def build(block, carry):
        at = pl.ds(pl.multiple_of(block * LANES, LANES), LANES)
        for ids, base, count in ((snd, 0, total), (rcv, total, nodes)):
            row = jnp.broadcast_to(ids[:, at], (LANES, LANES))
            column = jnp.transpose(row)
            for part in range(count // LANES):
                where = base + part * LANES
                pick[at, where : where + LANES] = one_hot(column == lane + part * LANES)
                put[where : where + LANES, at] = one_hot(row == sub + part * LANES)
        return carry

    lax.fori_loop(0, edges // LANES, build, 0)

    table[:nodes] = matmul(node[...], we1[width : 2 * width]).astype(bf16)
    table[nodes:total] = matmul(ghost[...], we1[width : 2 * width]).astype(bf16)
    table[total:] = matmul(node[...], we1[2 * width :]).astype(bf16)

    agg = jnp.zeros((nodes, width), f32)
    for start, size in split_tiles(edges // LANES, FORWARD_TILES):
        at = pl.ds(start, size)
        first = matmul(edge[at], we1[:width]) + matmul(pick[at], table[...]) + be[0:1]
        act, slope = silu_parts(first)
        z1 = act.astype(bf16)
        z1_s[at] = z1
        slope1_s[at] = slope
        act, slope = silu_parts(matmul(z1, weh[0]) + be[1:2])
        z2 = act.astype(bf16)
        z2_s[at] = z2
        slope2_s[at] = slope
        normed, inv = norm_parts(matmul(z2, weh[1]) + be[2:3])
        normed_s[at] = normed
        inv_s[at] = jnp.broadcast_to(inv, normed.shape)
        new = (normed * ge[...] + se[...]).astype(bf16)
        agg = agg + matmul(put[total:, at], new)

    agg = agg.astype(bf16)
    first = matmul(node[...], wn1[:width]) + matmul(agg, wn1[width:]) + bn[0:1]
    act, slope1 = silu_parts(first)
    z1 = act.astype(bf16)
    act, slope2 = silu_parts(matmul(z1, wnh[0]) + bn[1:2])
    z2 = act.astype(bf16)
    normed, inv = norm_parts(matmul(z2, wnh[1]) + bn[2:3])
    up = ncot[...].astype(f32)
    gain_row = rows_sum(up * normed)
    g3 = norm_back(up, gn[...], normed, inv)
    r3 = g3.astype(bf16)
    g2 = matmul_nt(r3, wnh[1]) * slope2
    r2 = g2.astype(bf16)
    g1 = matmul_nt(r2, wnh[0]) * slope1
    r1 = g1.astype(bf16)
    node_o[...] = up + matmul_nt(r1, wn1[:width])
    agg_grad = matmul_nt(r1, wn1[width:]).astype(bf16)
    node_terms = [contract_rows(node[...], r1), contract_rows(agg, r1)]
    node_terms += [contract_rows(z1, r2), contract_rows(z2, r3)]
    for index, term in enumerate(node_terms):
        npack[index * width : (index + 1) * width] = term * node_scale
    for pack, used in ((npack, 4 * width), (apack, 4 * width), (bpack, width)):
        if pack.shape[0] > used:
            pack[used:] = jnp.zeros((pack.shape[0] - used, width), f32)
    for index, row in enumerate((rows_sum(g1), rows_sum(g2), rows_sum(g3), gain_row)):
        bpack[width + 5 + index : width + 6 + index] = row * node_scale

    pl.semaphore_wait(barrier, len(greeted))
    node_red.scatter()

    small = [jnp.zeros((1, width), f32)] * 5
    acc = jnp.zeros((total + nodes, width), f32)
    grads = [jnp.zeros((width, width), f32)] * 3
    for number, (start, size) in enumerate(split_tiles(edges // LANES, BACKWARD_TILES)):
        at = pl.ds(start, size)
        up = ecot[at].astype(f32) + matmul(pick[at, total:], agg_grad)
        normed = normed_s[at]
        g3 = norm_back(up, ge[...], normed, inv_s[at])
        r3 = g3.astype(bf16)
        g2 = matmul_nt(r3, weh[1]) * slope2_s[at]
        r2 = g2.astype(bf16)
        g1 = matmul_nt(r2, weh[0]) * slope1_s[at]
        r1 = g1.astype(bf16)
        r1_s[at] = r1
        acc = acc + matmul(put[:, at], r1)
        grads[0] = grads[0] + contract_rows(edge[at], r1)
        grads[1] = grads[1] + contract_rows(z1_s[at], r2)
        grads[2] = grads[2] + contract_rows(z2_s[at], r3)
        for index, term in enumerate((g1, g2, g3, up * normed, up)):
            small[index] = small[index] + rows_sum(term)
        if number < 3:
            node_red.add()
            if number < 2:
                node_red.scatter()
            else:
                node_red.gather()

    by_sender = acc[:total].astype(bf16)
    by_receiver = acc[total:].astype(bf16)
    middle = contract_rows(node[...], by_sender[:nodes])
    middle = middle + contract_rows(ghost[...], by_sender[nodes:])
    last = contract_rows(node[...], by_receiver)
    for index, term in enumerate((grads[0], middle, last, grads[1])):
        apack[index * width : (index + 1) * width] = term * edge_scale
    bpack[:width] = grads[2] * edge_scale
    for index, row in enumerate(small):
        bpack[width + index : width + 1 + index] = row * edge_scale
    a_red.scatter()
    b_red.scatter()

    full = matmul_nt(by_sender, we1[width : 2 * width])
    ghost_s[...] = full[nodes:]
    halos = []
    for face in range(6):
        rows = pl.ds(face * slots, slots)
        copy = pltpu.make_async_remote_copy(
            src_ref=ghost_s.at[rows],
            dst_ref=halo.at[rows],
            send_sem=hsend.at[face],
            recv_sem=hland.at[face],
            device_id=face_target(sizes, face),
            device_id_type=MESH,
        )
        halos.append(copy)
    node_red.wait()
    a_red.add()
    b_red.add()
    a_red.scatter()
    b_red.scatter()
    node_red.gather()
    for copy in halos:
        copy.start()
    node_o[...] += full[:nodes] + matmul_nt(by_receiver, we1[2 * width :])
    half = edges // 2
    at = pl.ds(0, half)
    grad = ecot[at].astype(f32) + matmul_nt(r1_s[at], we1[:width])
    edge_o[at] = grad.astype(bf16)
    a_red.add()
    a_red.scatter()
    b_red.add()
    b_red.scatter()
    node_red.wait()
    node_red.gather()
    at = pl.ds(half, edges - half)
    grad = ecot[at].astype(f32) + matmul_nt(r1_s[at], we1[:width])
    edge_o[at] = grad.astype(bf16)
    a_red.add()
    a_red.gather()
    b_red.add()
    b_red.gather()
    for copy in halos:
        copy.wait()
    spot = lax.broadcasted_iota(jnp.int32, (nodes, slots), 0)
    local = node_o[...]
    for face in range(6):
        values = halo[face * slots : (face + 1) * slots].astype(bf16)
        local = local + matmul(one_hot(spot == faces[face]), values)
    node_o[...] = local
    a_red.wait()
    a_red.gather()
    b_red.wait()
    b_red.gather()
    node_red.wait()
    a_red.wait()
    a_red.gather()
    b_red.wait()
    b_red.gather()
    a_red.wait()
    b_red.wait()


def finish_kernel(
    node, edge, nred, ared, bred, node_o, edge_o, we1_o, weh_o, be_o, ge_o, se_o, wn1_o, wnh_o, bn_o, gn_o
):
    width = node.shape[1]
    node_o[...] = node[...]
    edge_o[...] = edge[...]
    we1_o[...] = ared[: 3 * width]
    weh_o[0] = ared[3 * width : 4 * width]
    weh_o[1] = bred[:width]
    wn1_o[...] = nred[: 2 * width]
    wnh_o[0] = nred[2 * width : 3 * width]
    wnh_o[1] = nred[3 * width : 4 * width]
    be_o[...] = bred[width : width + 3]
    ge_o[...] = bred[width + 3 : width + 4]
    se_o[...] = bred[width + 4 : width + 5]
    bn_o[...] = bred[width + 5 : width + 8]
    gn_o[...] = bred[width + 8 : width + 9]


VMEM = pl.BlockSpec(memory_space=pltpu.VMEM)


def on_device(
    sizes,
    node_latent,
    ghost_latent,
    edge_latent,
    senders,
    receivers,
    export_rows,
    node_cotangent,
    edge_cotangent,
    w_edge_in,
    w_edge_hidden,
    b_edge,
    gain_edge,
    shift_edge,
    w_node_in,
    w_node_hidden,
    b_node,
    gain_node,
):
    f32, bf16 = jnp.float32, jnp.bfloat16
    nodes, width = node_latent.shape[3:]
    slots = ghost_latent.shape[4]
    ghosts = 6 * slots
    edges = edge_latent.shape[3]
    total = nodes + ghosts
    devices = sizes["gx"] * sizes["gy"] * sizes["gz"]
    edge_scale = float(edges * devices) ** (-0.5)
    node_scale = float(nodes * devices) ** (-0.5)
    unit = 8 * devices

    def padded(rows):
        return -(-rows // unit) * unit

    def shape(*dims, dtype=f32):
        return jax.ShapeDtypeStruct(dims, dtype)

    core, near, far = stage_groups(sizes)
    four, two = padded(4 * width), padded(width + 9)
    reducers = reducer_scratch([core, near, far], four, width)
    reducers += reducer_scratch([core, near, far], four, width)
    reducers += reducer_scratch([core, far, near], two, width)
    passed = pl.pallas_call(
        functools.partial(block_kernel, sizes, edge_scale, node_scale),
        out_shape=(
            shape(nodes, width),
            shape(edges, width, dtype=bf16),
            shape(four, width),
            shape(four, width),
            shape(two, width),
        ),
        in_specs=[VMEM] * 17,
        out_specs=(VMEM,) * 5,
        scratch_shapes=[
            pltpu.VMEM((edges, total + nodes), bf16),
            pltpu.VMEM((total + nodes, edges), bf16),
            pltpu.VMEM((total + nodes, width), bf16),
            pltpu.VMEM((edges, width), bf16),
            pltpu.VMEM((edges, width), bf16),
            pltpu.VMEM((edges, width), bf16),
            pltpu.VMEM((edges, width), f32),
            pltpu.VMEM((edges, width), f32),
            pltpu.VMEM((edges, width), f32),
            pltpu.VMEM((edges, width), f32),
            pltpu.VMEM((four, width), f32),
            pltpu.VMEM((four, width), f32),
            pltpu.VMEM((two, width), f32),
            pltpu.VMEM((ghosts, width), f32),
            pltpu.VMEM((ghosts, width), f32),
            pltpu.SemaphoreType.DMA((6,)),
            pltpu.SemaphoreType.DMA((6,)),
        ]
        + reducers,
        compiler_params=pltpu.CompilerParams(
            collective_id=0, has_side_effects=True, vmem_limit_bytes=60 * 1024 * 1024
        ),
        name="block_pass",
    )(
        node_latent.reshape(nodes, width),
        ghost_latent.reshape(ghosts, width),
        edge_latent.reshape(edges, width),
        senders.reshape(1, edges),
        receivers.reshape(1, edges),
        export_rows.reshape(6, 1, slots),
        node_cotangent.reshape(nodes, width),
        edge_cotangent.reshape(edges, width),
        w_edge_in,
        w_edge_hidden,
        b_edge,
        gain_edge.reshape(1, width),
        shift_edge.reshape(1, width),
        w_node_in,
        w_node_hidden,
        b_node,
        gain_node.reshape(1, width),
    )

    outs = pl.pallas_call(
        finish_kernel,
        out_shape=(
            shape(nodes, width),
            shape(edges, width, dtype=bf16),
            shape(3 * width, width),
            shape(2, width, width),
            shape(3, width),
            shape(1, width),
            shape(1, width),
            shape(2 * width, width),
            shape(2, width, width),
            shape(3, width),
            shape(1, width),
        ),
        in_specs=[VMEM] * 5,
        out_specs=(VMEM,) * 11,
        name="finish",
    )(*passed)
    node_grad, edge_grad, we1, weh, be, ge, se, wn1, wnh, bn, gn = outs
    return (
        node_grad.reshape(node_latent.shape),
        edge_grad.reshape(edge_latent.shape),
        we1,
        weh,
        be,
        ge.reshape(width),
        se.reshape(width),
        wn1,
        wnh,
        bn,
        gn.reshape(width),
    )


def solution(mesh):
    block = P("gx", "gy", "gz")
    sizes = dict(mesh.shape)
    return jax.shard_map(
        functools.partial(on_device, sizes),
        mesh=mesh,
        in_specs=(block,) * 8 + (P(),) * 9,
        out_specs=(block,) * 2 + (P(),) * 9,
        check_vma=False,
    )
```

```python
import functools

import jax
import jax.numpy as jnp
from jax import lax
from jax.experimental import pallas as pl
from jax.experimental.pallas import tpu as pltpu
from jax.sharding import PartitionSpec as P

EPSILON = 1e-05
LANES = 128
FORWARD_TILES = 2
BACKWARD_TILES = 4
MESH = pl.DeviceIdType.MESH
AXES = ("gx", "gy", "gz")


def matmul(left, right):
    return jnp.dot(left, right, preferred_element_type=jnp.float32)


def matmul_nt(left, right):
    return lax.dot_general(
        left, right, (((1,), (1,)), ((), ())), preferred_element_type=jnp.float32
    )


def contract_rows(left, right):
    return lax.dot_general(
        left, right, (((0,), (0,)), ((), ())), preferred_element_type=jnp.float32
    )


def silu_parts(preact):
    sigmoid = 0.5 * jnp.tanh(0.5 * preact) + 0.5
    act = preact * sigmoid
    return act, sigmoid + act * (1.0 - sigmoid)


def norm_parts(preact):
    centred = preact - jnp.mean(preact, -1, keepdims=True)
    inv_std = lax.rsqrt(jnp.mean(centred * centred, -1, keepdims=True) + EPSILON)
    return centred * inv_std, inv_std


def norm_back(grad_out, gain, normed, inv_std):
    scaled = grad_out * gain
    return inv_std * (
        scaled
        - jnp.mean(scaled, -1, keepdims=True)
        - normed * jnp.mean(scaled * normed, -1, keepdims=True)
    )


def rows_sum(values):
    return jnp.sum(values, 0, keepdims=True)


def one_hot(hit):
    return jnp.where(hit, 1.0, 0.0).astype(jnp.bfloat16)


def stage_groups(sizes):
    near = [("gx", sizes["gx"], 1), ("gz", sizes["gz"], 1)]
    far = [("gy", sizes["gy"], 1)]
    return near, far


def group_size(group):
    count = 1
    for _, members, _ in group:
        count *= members
    return count


def coordinate(part):
    axis, count, stride = part
    return lax.rem(lax.axis_index(axis) // stride, count)


def member(group):
    index = 0
    for part in group:
        index = index * part[1] + coordinate(part)
    return index


def peers(group):
    steps = [()]
    for part in group:
        steps = [step + (more,) for step in steps for more in range(part[1])]
    found = []
    for step in steps[1:]:
        index = 0
        device = {}
        for part, more in zip(group, step):
            axis, count, stride = part
            mine = coordinate(part)
            other = lax.rem(mine + more, count)
            index = index * count + other
            here = device.get(axis, lax.axis_index(axis))
            device[axis] = here + (other - mine) * stride
        found.append((index, device))
    return found


class Reducer:
    def __init__(self, groups, source, out, scratch):
        self.groups = groups
        self.out = out
        self.source = source
        count = len(groups)
        self.landing = scratch[:count]
        self.sums = scratch[count : 2 * count]
        self.sems = scratch[2 * count :]
        self.length = source.shape[0]
        self.offset = 0
        self.segments = []
        self.slot = 0
        self.pending = []

    def send(self, source, target, device, sends, lands):
        copy = pltpu.make_async_remote_copy(
            src_ref=source,
            dst_ref=target,
            send_sem=self.sems[sends].at[self.slot],
            recv_sem=self.sems[lands].at[self.slot],
            device_id=device,
            device_id_type=MESH,
        )
        copy.start()
        self.pending.append(copy)
        self.slot += 1

    def wait(self):
        for copy in self.pending:
            copy.wait()
        self.pending = []

    def scatter(self):
        index = len(self.segments)
        group = self.groups[index]
        piece = self.length // group_size(group)
        for spot, (other, device) in enumerate(peers(group)):
            rows = pl.ds(pl.multiple_of(other * piece, 8), piece)
            self.send(self.source.at[rows], self.landing[index].at[spot], device, 0, 1)

    def add(self):
        index = len(self.segments)
        group = self.groups[index]
        piece = self.length // group_size(group)
        self.wait()
        mine = member(group)
        total = self.source[pl.ds(pl.multiple_of(mine * piece, 8), piece)]
        for spot in range(group_size(group) - 1):
            total = total + self.landing[index][spot]
        self.offset = self.offset + mine * piece
        self.segments.append((group, self.offset, piece))
        if len(self.segments) == len(self.groups):
            self.out[pl.ds(pl.multiple_of(self.offset, 8), piece)] = total
            self.slot = 0
        else:
            self.sums[index][...] = total
            self.source = self.sums[index]
            self.length = piece

    def gather(self):
        group, start, piece = self.segments.pop()
        rows = pl.ds(pl.multiple_of(start, 8), piece)
        for _, device in peers(group):
            self.send(self.out.at[rows], self.out.at[rows], device, 2, 3)


def reducer_scratch(groups, rows, width):
    landing, sums, hops = [], [], 0
    for group in groups:
        rows //= group_size(group)
        landing.append(pltpu.VMEM((group_size(group) - 1, rows, width), jnp.float32))
        sums.append(pltpu.VMEM((rows, width), jnp.float32))
        hops += group_size(group) - 1
    return landing + sums + [pltpu.SemaphoreType.DMA((hops,))] * 4


def split_tiles(blocks, tiles):
    sizes = [blocks // tiles + (index < blocks % tiles) for index in range(tiles)]
    starts = [sum(sizes[:index]) for index in range(tiles)]
    return [(LANES * start, LANES * size) for start, size in zip(starts, sizes)]


def face_target(sizes, face):
    axis, side = AXES[face // 2], face % 2
    count = sizes[axis]
    step = 1 if side == 0 else count - 1
    return {axis: lax.rem(lax.axis_index(axis) + step, count)}


def block_kernel(
    sizes,
    edge_scale,
    node_scale,
    node,
    ghost,
    edge,
    snd,
    rcv,
    faces,
    ncot,
    ecot,
    we1,
    weh,
    be,
    ge,
    se,
    wn1,
    wnh,
    bn,
    gn,
    node_o,
    edge_o,
    nred_o,
    ared_o,
    bred_o,
    pick,
    put,
    table,
    z1_s,
    z2_s,
    r1_s,
    slope1_s,
    slope2_s,
    normed_s,
    inv_s,
    npack,
    apack,
    bpack,
    edge_s,
    ecot_s,
    ghost_s,
    halo,
    loads,
    hsend,
    hland,
    *scratch,
):
    nodes, width = node.shape
    edges = edge.shape[0]
    ghosts = ghost.shape[0]
    slots = ghosts // 6
    total = nodes + ghosts
    bf16, f32 = jnp.bfloat16, jnp.float32
    near, far = stage_groups(sizes)
    third = len(scratch) // 3
    node_red = Reducer([near, far], npack, nred_o, scratch[:third])
    a_red = Reducer([near, far], apack, ared_o, scratch[third : 2 * third])
    b_red = Reducer([far, near], bpack, bred_o, scratch[2 * third :])

    loaded = [
        pltpu.make_async_copy(edge, edge_s, loads.at[0]),
        pltpu.make_async_copy(ecot, ecot_s, loads.at[1]),
    ]
    for copy in loaded:
        copy.start()
    barrier = pltpu.get_barrier_semaphore()
    greeted = [face_target(sizes, face) for face in range(6)]
    for group in (near, far):
        greeted += [device for _, device in peers(group)]
    for device in greeted:
        pl.semaphore_signal(barrier, inc=1, device_id=device, device_id_type=MESH)

    lane = lax.broadcasted_iota(jnp.int32, (LANES, LANES), 1).astype(jnp.int16)
    sub = lax.broadcasted_iota(jnp.int32, (LANES, LANES), 0).astype(jnp.int16)
    one = jnp.ones((LANES, LANES), bf16)
    zero = jnp.zeros((LANES, LANES), bf16)

    def build(block, carry):
        at = pl.ds(pl.multiple_of(block * LANES, LANES), LANES)
        for ids, base, count in ((snd, 0, total), (rcv, total, nodes)):
            row = jnp.broadcast_to(ids[:, at], (LANES, LANES))
            column = jnp.transpose(row).astype(jnp.int16)
            row = row.astype(jnp.int16)
            for part in range(count // LANES):
                where = base + part * LANES
                pick[at, where : where + LANES] = jnp.where(
                    column == lane + jnp.int16(part * LANES), one, zero
                )
                put[where : where + LANES, at] = jnp.where(
                    row == sub + jnp.int16(part * LANES), one, zero
                )
        return carry

    lax.fori_loop(0, edges // LANES, build, 0)

    table[:nodes] = matmul(node[...], we1[width : 2 * width]).astype(bf16)
    table[nodes:total] = matmul(ghost[...], we1[width : 2 * width]).astype(bf16)
    table[total:] = matmul(node[...], we1[2 * width :]).astype(bf16)

    loaded[0].wait()
    agg = jnp.zeros((nodes, width), f32)
    for start, size in split_tiles(edges // LANES, FORWARD_TILES):
        at = pl.ds(start, size)
        first = matmul(edge_s[at], we1[:width]) + matmul(pick[at], table[...]) + be[0:1]
        act, slope = silu_parts(first)
        z1 = act.astype(bf16)
        z1_s[at] = z1
        slope1_s[at] = slope
        act, slope = silu_parts(matmul(z1, weh[0]) + be[1:2])
        z2 = act.astype(bf16)
        z2_s[at] = z2
        slope2_s[at] = slope
        normed, inv = norm_parts(matmul(z2, weh[1]) + be[2:3])
        normed_s[at] = normed
        inv_s[at] = jnp.broadcast_to(inv, normed.shape)
        new = (normed * ge[...] + se[...]).astype(bf16)
        agg = agg + matmul(put[total:, at], new)

    agg = agg.astype(bf16)
    first = matmul(node[...], wn1[:width]) + matmul(agg, wn1[width:]) + bn[0:1]
    act, slope1 = silu_parts(first)
    z1 = act.astype(bf16)
    act, slope2 = silu_parts(matmul(z1, wnh[0]) + bn[1:2])
    z2 = act.astype(bf16)
    normed, inv = norm_parts(matmul(z2, wnh[1]) + bn[2:3])
    up = ncot[...].astype(f32)
    gain_row = rows_sum(up * normed)
    g3 = norm_back(up, gn[...], normed, inv)
    r3 = g3.astype(bf16)
    g2 = matmul_nt(r3, wnh[1]) * slope2
    r2 = g2.astype(bf16)
    g1 = matmul_nt(r2, wnh[0]) * slope1
    r1 = g1.astype(bf16)
    node_o[...] = up + matmul_nt(r1, wn1[:width])
    agg_grad = matmul_nt(r1, wn1[width:]).astype(bf16)
    node_terms = [contract_rows(node[...], r1), contract_rows(agg, r1)]
    node_terms += [contract_rows(z1, r2), contract_rows(z2, r3)]
    for index, term in enumerate(node_terms):
        npack[index * width : (index + 1) * width] = term * node_scale
    for pack, used in ((npack, 4 * width), (apack, 4 * width), (bpack, width)):
        if pack.shape[0] > used:
            pack[used:] = jnp.zeros((pack.shape[0] - used, width), f32)
    for index, row in enumerate((rows_sum(g1), rows_sum(g2), rows_sum(g3), gain_row)):
        bpack[width + 5 + index : width + 6 + index] = row * node_scale

    pl.semaphore_wait(barrier, len(greeted))
    node_red.scatter()

    loaded[1].wait()
    small = [jnp.zeros((1, width), f32)] * 5
    acc = jnp.zeros((total + nodes, width), f32)
    grads = [jnp.zeros((width, width), f32)] * 3
    for number, (start, size) in enumerate(split_tiles(edges // LANES, BACKWARD_TILES)):
        at = pl.ds(start, size)
        up = ecot_s[at].astype(f32) + matmul(pick[at, total:], agg_grad)
        normed = normed_s[at]
        g3 = norm_back(up, ge[...], normed, inv_s[at])
        r3 = g3.astype(bf16)
        g2 = matmul_nt(r3, weh[1]) * slope2_s[at]
        r2 = g2.astype(bf16)
        g1 = matmul_nt(r2, weh[0]) * slope1_s[at]
        r1 = g1.astype(bf16)
        r1_s[at] = r1
        acc = acc + matmul(put[:, at], r1)
        grads[0] = grads[0] + contract_rows(edge_s[at], r1)
        grads[1] = grads[1] + contract_rows(z1_s[at], r2)
        grads[2] = grads[2] + contract_rows(z2_s[at], r3)
        for index, term in enumerate((g1, g2, g3, up * normed, up)):
            small[index] = small[index] + rows_sum(term)

    by_sender = acc[:total].astype(bf16)
    by_receiver = acc[total:].astype(bf16)
    middle = contract_rows(node[...], by_sender[:nodes])
    middle = middle + contract_rows(ghost[...], by_sender[nodes:])
    last = contract_rows(node[...], by_receiver)
    for index, term in enumerate((grads[0], middle, last, grads[1])):
        apack[index * width : (index + 1) * width] = term * edge_scale
    bpack[:width] = grads[2] * edge_scale
    for index, row in enumerate(small):
        bpack[width + index : width + 1 + index] = row * edge_scale
    a_red.scatter()
    b_red.scatter()
    node_red.add()
    node_red.scatter()

    full = matmul_nt(by_sender, we1[width : 2 * width])
    ghost_s[...] = full[nodes:]
    halos = []
    for face in range(6):
        rows = pl.ds(face * slots, slots)
        copy = pltpu.make_async_remote_copy(
            src_ref=ghost_s.at[rows],
            dst_ref=halo.at[rows],
            send_sem=hsend.at[face],
            recv_sem=hland.at[face],
            device_id=face_target(sizes, face),
            device_id_type=MESH,
        )
        copy.start()
        halos.append(copy)
    node_o[...] += full[:nodes] + matmul_nt(by_receiver, we1[2 * width :])
    half = edges // 2
    at = pl.ds(0, half)
    grad = ecot_s[at].astype(f32) + matmul_nt(r1_s[at], we1[:width])
    edge_o[at] = grad.astype(bf16)
    a_red.add()
    a_red.scatter()
    b_red.add()
    b_red.scatter()
    node_red.add()
    node_red.gather()
    at = pl.ds(half, edges - half)
    grad = ecot_s[at].astype(f32) + matmul_nt(r1_s[at], we1[:width])
    edge_o[at] = grad.astype(bf16)
    a_red.add()
    a_red.gather()
    b_red.add()
    b_red.gather()
    node_red.wait()
    node_red.gather()
    for copy in halos:
        copy.wait()
    spot = lax.broadcasted_iota(jnp.int32, (nodes, slots), 0)
    local = node_o[...]
    for face in range(6):
        values = halo[face * slots : (face + 1) * slots].astype(bf16)
        local = local + matmul(one_hot(spot == faces[face]), values)
    node_o[...] = local
    a_red.wait()
    a_red.gather()
    b_red.wait()
    b_red.gather()
    node_red.wait()
    a_red.wait()
    b_red.wait()


def finish_kernel(
    node, edge, nred, ared, bred, node_o, edge_o, we1_o, weh_o, be_o, ge_o, se_o, wn1_o, wnh_o, bn_o, gn_o
):
    width = node.shape[1]
    node_o[...] = node[...]
    edge_o[...] = edge[...]
    we1_o[...] = ared[: 3 * width]
    weh_o[0] = ared[3 * width : 4 * width]
    weh_o[1] = bred[:width]
    wn1_o[...] = nred[: 2 * width]
    wnh_o[0] = nred[2 * width : 3 * width]
    wnh_o[1] = nred[3 * width : 4 * width]
    be_o[...] = bred[width : width + 3]
    ge_o[...] = bred[width + 3 : width + 4]
    se_o[...] = bred[width + 4 : width + 5]
    bn_o[...] = bred[width + 5 : width + 8]
    gn_o[...] = bred[width + 8 : width + 9]


VMEM = pl.BlockSpec(memory_space=pltpu.VMEM)
HBM = pl.BlockSpec(memory_space=pl.ANY)


def on_device(
    sizes,
    node_latent,
    ghost_latent,
    edge_latent,
    senders,
    receivers,
    export_rows,
    node_cotangent,
    edge_cotangent,
    w_edge_in,
    w_edge_hidden,
    b_edge,
    gain_edge,
    shift_edge,
    w_node_in,
    w_node_hidden,
    b_node,
    gain_node,
):
    f32, bf16 = jnp.float32, jnp.bfloat16
    nodes, width = node_latent.shape[3:]
    slots = ghost_latent.shape[4]
    ghosts = 6 * slots
    edges = edge_latent.shape[3]
    total = nodes + ghosts
    devices = sizes["gx"] * sizes["gy"] * sizes["gz"]
    edge_scale = float(edges * devices) ** (-0.5)
    node_scale = float(nodes * devices) ** (-0.5)
    unit = 8 * devices

    def padded(rows):
        return -(-rows // unit) * unit

    def shape(*dims, dtype=f32):
        return jax.ShapeDtypeStruct(dims, dtype)

    near, far = stage_groups(sizes)
    four, two = padded(4 * width), padded(width + 9)
    reducers = reducer_scratch([near, far], four, width)
    reducers += reducer_scratch([near, far], four, width)
    reducers += reducer_scratch([far, near], two, width)
    passed = pl.pallas_call(
        functools.partial(block_kernel, sizes, edge_scale, node_scale),
        out_shape=(
            shape(nodes, width),
            shape(edges, width, dtype=bf16),
            shape(four, width),
            shape(four, width),
            shape(two, width),
        ),
        in_specs=[VMEM] * 2 + [HBM] + [VMEM] * 4 + [HBM] + [VMEM] * 9,
        out_specs=(VMEM,) * 5,
        scratch_shapes=[
            pltpu.VMEM((edges, total + nodes), bf16),
            pltpu.VMEM((total + nodes, edges), bf16),
            pltpu.VMEM((total + nodes, width), bf16),
            pltpu.VMEM((edges, width), bf16),
            pltpu.VMEM((edges, width), bf16),
            pltpu.VMEM((edges, width), bf16),
            pltpu.VMEM((edges, width), f32),
            pltpu.VMEM((edges, width), f32),
            pltpu.VMEM((edges, width), f32),
            pltpu.VMEM((edges, width), f32),
            pltpu.VMEM((four, width), f32),
            pltpu.VMEM((four, width), f32),
            pltpu.VMEM((two, width), f32),
            pltpu.VMEM((edges, width), bf16),
            pltpu.VMEM((edges, width), bf16),
            pltpu.VMEM((ghosts, width), f32),
            pltpu.VMEM((ghosts, width), f32),
            pltpu.SemaphoreType.DMA((2,)),
            pltpu.SemaphoreType.DMA((6,)),
            pltpu.SemaphoreType.DMA((6,)),
        ]
        + reducers,
        compiler_params=pltpu.CompilerParams(
            collective_id=0, has_side_effects=True, vmem_limit_bytes=60 * 1024 * 1024
        ),
        name="block_pass",
    )(
        node_latent.reshape(nodes, width),
        ghost_latent.reshape(ghosts, width),
        edge_latent.reshape(edges, width),
        senders.reshape(1, edges),
        receivers.reshape(1, edges),
        export_rows.reshape(6, 1, slots),
        node_cotangent.reshape(nodes, width),
        edge_cotangent.reshape(edges, width),
        w_edge_in,
        w_edge_hidden,
        b_edge,
        gain_edge.reshape(1, width),
        shift_edge.reshape(1, width),
        w_node_in,
        w_node_hidden,
        b_node,
        gain_node.reshape(1, width),
    )

    outs = pl.pallas_call(
        finish_kernel,
        out_shape=(
            shape(nodes, width),
            shape(edges, width, dtype=bf16),
            shape(3 * width, width),
            shape(2, width, width),
            shape(3, width),
            shape(1, width),
            shape(1, width),
            shape(2 * width, width),
            shape(2, width, width),
            shape(3, width),
            shape(1, width),
        ),
        in_specs=[VMEM] * 5,
        out_specs=(VMEM,) * 11,
        name="finish",
    )(*passed)
    node_grad, edge_grad, we1, weh, be, ge, se, wn1, wnh, bn, gn = outs
    return (
        node_grad.reshape(node_latent.shape),
        edge_grad.reshape(edge_latent.shape),
        we1,
        weh,
        be,
        ge.reshape(width),
        se.reshape(width),
        wn1,
        wnh,
        bn,
        gn.reshape(width),
    )


def solution(mesh):
    block = P("gx", "gy", "gz")
    sizes = dict(mesh.shape)
    return jax.shard_map(
        functools.partial(on_device, sizes),
        mesh=mesh,
        in_specs=(block,) * 8 + (P(),) * 9,
        out_specs=(block,) * 2 + (P(),) * 9,
        check_vma=False,
    )
```

```python
import functools

import jax
import jax.numpy as jnp
from jax import lax
from jax.experimental import pallas as pl
from jax.experimental.pallas import tpu as pltpu
from jax.sharding import PartitionSpec as P

EPSILON = 1e-05
LANES = 128
FORWARD_TILES = 2
BACKWARD_TILES = 4
MESH = pl.DeviceIdType.MESH
AXES = ("gx", "gy", "gz")


def matmul(left, right):
    return jnp.dot(left, right, preferred_element_type=jnp.float32)


def matmul_nt(left, right):
    return lax.dot_general(
        left, right, (((1,), (1,)), ((), ())), preferred_element_type=jnp.float32
    )


def contract_rows(left, right):
    return lax.dot_general(
        left, right, (((0,), (0,)), ((), ())), preferred_element_type=jnp.float32
    )


def silu_parts(preact):
    sigmoid = 0.5 * jnp.tanh(0.5 * preact) + 0.5
    act = preact * sigmoid
    return act, sigmoid + act * (1.0 - sigmoid)


def norm_parts(preact):
    centred = preact - jnp.mean(preact, -1, keepdims=True)
    inv_std = lax.rsqrt(jnp.mean(centred * centred, -1, keepdims=True) + EPSILON)
    return centred * inv_std, inv_std


def norm_back(grad_out, gain, normed, inv_std):
    scaled = grad_out * gain
    return inv_std * (
        scaled
        - jnp.mean(scaled, -1, keepdims=True)
        - normed * jnp.mean(scaled * normed, -1, keepdims=True)
    )


def rows_sum(values):
    return jnp.sum(values, 0, keepdims=True)


def one_hot(hit):
    return jnp.where(hit, 1.0, 0.0).astype(jnp.bfloat16)


def stage_groups(sizes):
    near = [("gx", sizes["gx"], 1), ("gz", sizes["gz"], 1)]
    far = [("gy", sizes["gy"], 1)]
    return near, far


def group_size(group):
    count = 1
    for _, members, _ in group:
        count *= members
    return count


def coordinate(part):
    axis, count, stride = part
    return lax.rem(lax.axis_index(axis) // stride, count)


def member(group):
    index = 0
    for part in group:
        index = index * part[1] + coordinate(part)
    return index


def peers(group):
    steps = [()]
    for part in group:
        steps = [step + (more,) for step in steps for more in range(part[1])]
    found = []
    for step in steps[1:]:
        index = 0
        device = {}
        for part, more in zip(group, step):
            axis, count, stride = part
            mine = coordinate(part)
            other = lax.rem(mine + more, count)
            index = index * count + other
            here = device.get(axis, lax.axis_index(axis))
            device[axis] = here + (other - mine) * stride
        found.append((index, device))
    return found


class Reducer:
    def __init__(self, first, second, source, out, scratch):
        self.first, self.second = first, second
        self.source, self.out = source, out
        self.landing, self.swap, self.part = scratch[:3]
        self.sems = scratch[3:]
        self.piece = source.shape[0] // group_size(first)
        self.home = pl.ds(pl.multiple_of(member(first) * self.piece, 8), self.piece)
        self.pending = []

    def send(self, source, target, device, spot, stage):
        copy = pltpu.make_async_remote_copy(
            src_ref=source,
            dst_ref=target,
            send_sem=self.sems[2 * stage].at[spot],
            recv_sem=self.sems[2 * stage + 1].at[spot],
            device_id=device,
            device_id_type=MESH,
        )
        copy.start()
        self.pending.append(copy)

    def wait(self):
        for copy in self.pending:
            copy.wait()
        self.pending = []

    def scatter(self):
        for spot, (other, device) in enumerate(peers(self.first)):
            rows = pl.ds(pl.multiple_of(other * self.piece, 8), self.piece)
            self.send(self.source.at[rows], self.landing.at[spot], device, spot, 0)

    def exchange(self):
        self.wait()
        total = self.source[self.home]
        for spot in range(group_size(self.first) - 1):
            total = total + self.landing[spot]
        mine = member(self.second)
        self.part[...] = total
        self.swap[mine] = total
        for spot, (_, device) in enumerate(peers(self.second)):
            self.send(self.part, self.swap.at[mine], device, spot, 1)

    def gather(self):
        self.wait()
        total = self.swap[0]
        for index in range(1, group_size(self.second)):
            total = total + self.swap[index]
        self.out[self.home] = total
        for spot, (_, device) in enumerate(peers(self.first)):
            self.send(self.out.at[self.home], self.out.at[self.home], device, spot, 2)


def reducer_scratch(first, second, rows, width):
    one, two = group_size(first), group_size(second)
    piece = rows // one
    dma = pltpu.SemaphoreType.DMA
    return [
        pltpu.VMEM((one - 1, piece, width), jnp.float32),
        pltpu.VMEM((two, piece, width), jnp.float32),
        pltpu.VMEM((piece, width), jnp.float32),
        dma((one - 1,)),
        dma((one - 1,)),
        dma((two - 1,)),
        dma((two - 1,)),
        dma((one - 1,)),
        dma((one - 1,)),
    ]


def split_tiles(blocks, tiles):
    sizes = [blocks // tiles + (index < blocks % tiles) for index in range(tiles)]
    starts = [sum(sizes[:index]) for index in range(tiles)]
    return [(LANES * start, LANES * size) for start, size in zip(starts, sizes)]


def face_target(sizes, face):
    axis, side = AXES[face // 2], face % 2
    count = sizes[axis]
    step = 1 if side == 0 else count - 1
    return {axis: lax.rem(lax.axis_index(axis) + step, count)}


def block_kernel(
    sizes,
    edge_scale,
    node_scale,
    node,
    ghost,
    edge,
    snd,
    rcv,
    faces,
    ncot,
    ecot,
    we1,
    weh,
    be,
    ge,
    se,
    wn1,
    wnh,
    bn,
    gn,
    node_o,
    edge_o,
    nred_o,
    ared_o,
    bred_o,
    pick,
    put,
    table,
    z1_s,
    z2_s,
    r1_s,
    slope1_s,
    slope2_s,
    normed_s,
    inv_s,
    npack,
    apack,
    bpack,
    edge_s,
    ecot_s,
    ghost_s,
    halo,
    loads,
    hsend,
    hland,
    *scratch,
):
    nodes, width = node.shape
    edges = edge.shape[0]
    ghosts = ghost.shape[0]
    slots = ghosts // 6
    total = nodes + ghosts
    bf16, f32 = jnp.bfloat16, jnp.float32
    near, far = stage_groups(sizes)
    third = len(scratch) // 3
    node_red = Reducer(near, far, npack, nred_o, scratch[:third])
    a_red = Reducer(near, far, apack, ared_o, scratch[third : 2 * third])
    b_red = Reducer(far, near, bpack, bred_o, scratch[2 * third :])

    loaded = [
        pltpu.make_async_copy(edge, edge_s, loads.at[0]),
        pltpu.make_async_copy(ecot, ecot_s, loads.at[1]),
    ]
    for copy in loaded:
        copy.start()
    barrier = pltpu.get_barrier_semaphore()
    greeted = [face_target(sizes, face) for face in range(6)]
    for group in (near, far):
        greeted += [device for _, device in peers(group)]
    for device in greeted:
        pl.semaphore_signal(barrier, inc=1, device_id=device, device_id_type=MESH)

    lane = lax.broadcasted_iota(jnp.int32, (LANES, LANES), 1).astype(jnp.int16)
    sub = lax.broadcasted_iota(jnp.int32, (LANES, LANES), 0).astype(jnp.int16)
    one = jnp.ones((LANES, LANES), bf16)
    zero = jnp.zeros((LANES, LANES), bf16)

    def build(block, carry):
        at = pl.ds(pl.multiple_of(block * LANES, LANES), LANES)
        for ids, base, count in ((snd, 0, total), (rcv, total, nodes)):
            row = jnp.broadcast_to(ids[:, at], (LANES, LANES))
            column = jnp.transpose(row).astype(jnp.int16)
            row = row.astype(jnp.int16)
            for part in range(count // LANES):
                where = base + part * LANES
                pick[at, where : where + LANES] = jnp.where(
                    column == lane + jnp.int16(part * LANES), one, zero
                )
                put[where : where + LANES, at] = jnp.where(
                    row == sub + jnp.int16(part * LANES), one, zero
                )
        return carry

    lax.fori_loop(0, edges // LANES, build, 0)

    table[:nodes] = matmul(node[...], we1[width : 2 * width]).astype(bf16)
    table[nodes:total] = matmul(ghost[...], we1[width : 2 * width]).astype(bf16)
    table[total:] = matmul(node[...], we1[2 * width :]).astype(bf16)

    loaded[0].wait()
    agg = jnp.zeros((nodes, width), f32)
    for start, size in split_tiles(edges // LANES, FORWARD_TILES):
        at = pl.ds(start, size)
        first = matmul(edge_s[at], we1[:width]) + matmul(pick[at], table[...]) + be[0:1]
        act, slope = silu_parts(first)
        z1 = act.astype(bf16)
        z1_s[at] = z1
        slope1_s[at] = slope
        act, slope = silu_parts(matmul(z1, weh[0]) + be[1:2])
        z2 = act.astype(bf16)
        z2_s[at] = z2
        slope2_s[at] = slope
        normed, inv = norm_parts(matmul(z2, weh[1]) + be[2:3])
        normed_s[at] = normed
        inv_s[at] = jnp.broadcast_to(inv, normed.shape)
        new = (normed * ge[...] + se[...]).astype(bf16)
        agg = agg + matmul(put[total:, at], new)

    agg = agg.astype(bf16)
    first = matmul(node[...], wn1[:width]) + matmul(agg, wn1[width:]) + bn[0:1]
    act, slope1 = silu_parts(first)
    z1 = act.astype(bf16)
    act, slope2 = silu_parts(matmul(z1, wnh[0]) + bn[1:2])
    z2 = act.astype(bf16)
    normed, inv = norm_parts(matmul(z2, wnh[1]) + bn[2:3])
    up = ncot[...].astype(f32)
    gain_row = rows_sum(up * normed)
    g3 = norm_back(up, gn[...], normed, inv)
    r3 = g3.astype(bf16)
    g2 = matmul_nt(r3, wnh[1]) * slope2
    r2 = g2.astype(bf16)
    g1 = matmul_nt(r2, wnh[0]) * slope1
    r1 = g1.astype(bf16)
    node_o[...] = up + matmul_nt(r1, wn1[:width])
    agg_grad = matmul_nt(r1, wn1[width:]).astype(bf16)
    node_terms = [contract_rows(node[...], r1), contract_rows(agg, r1)]
    node_terms += [contract_rows(z1, r2), contract_rows(z2, r3)]
    for index, term in enumerate(node_terms):
        npack[index * width : (index + 1) * width] = term * node_scale
    for pack, used in ((npack, 4 * width), (apack, 4 * width), (bpack, width)):
        if pack.shape[0] > used:
            pack[used:] = jnp.zeros((pack.shape[0] - used, width), f32)
    for index, row in enumerate((rows_sum(g1), rows_sum(g2), rows_sum(g3), gain_row)):
        bpack[width + 5 + index : width + 6 + index] = row * node_scale

    pl.semaphore_wait(barrier, len(greeted))
    node_red.scatter()

    loaded[1].wait()
    small = [jnp.zeros((1, width), f32)] * 5
    acc = jnp.zeros((total + nodes, width), f32)
    grads = [jnp.zeros((width, width), f32)] * 3
    for number, (start, size) in enumerate(split_tiles(edges // LANES, BACKWARD_TILES)):
        at = pl.ds(start, size)
        up = ecot_s[at].astype(f32) + matmul(pick[at, total:], agg_grad)
        normed = normed_s[at]
        g3 = norm_back(up, ge[...], normed, inv_s[at])
        r3 = g3.astype(bf16)
        g2 = matmul_nt(r3, weh[1]) * slope2_s[at]
        r2 = g2.astype(bf16)
        g1 = matmul_nt(r2, weh[0]) * slope1_s[at]
        r1 = g1.astype(bf16)
        r1_s[at] = r1
        acc = acc + matmul(put[:, at], r1)
        grads[0] = grads[0] + contract_rows(edge_s[at], r1)
        grads[1] = grads[1] + contract_rows(z1_s[at], r2)
        grads[2] = grads[2] + contract_rows(z2_s[at], r3)
        for index, term in enumerate((g1, g2, g3, up * normed, up)):
            small[index] = small[index] + rows_sum(term)

    by_sender = acc[:total].astype(bf16)
    by_receiver = acc[total:].astype(bf16)
    middle = contract_rows(node[...], by_sender[:nodes])
    middle = middle + contract_rows(ghost[...], by_sender[nodes:])
    last = contract_rows(node[...], by_receiver)
    for index, term in enumerate((grads[0], middle, last, grads[1])):
        apack[index * width : (index + 1) * width] = term * edge_scale
    bpack[:width] = grads[2] * edge_scale
    for index, row in enumerate(small):
        bpack[width + index : width + 1 + index] = row * edge_scale
    a_red.scatter()
    b_red.scatter()
    node_red.exchange()

    full = matmul_nt(by_sender, we1[width : 2 * width])
    ghost_s[...] = full[nodes:]
    halos = []
    for face in range(6):
        rows = pl.ds(face * slots, slots)
        copy = pltpu.make_async_remote_copy(
            src_ref=ghost_s.at[rows],
            dst_ref=halo.at[rows],
            send_sem=hsend.at[face],
            recv_sem=hland.at[face],
            device_id=face_target(sizes, face),
            device_id_type=MESH,
        )
        copy.start()
        halos.append(copy)
    node_o[...] += full[:nodes] + matmul_nt(by_receiver, we1[2 * width :])
    half = edges // 2
    at = pl.ds(0, half)
    grad = ecot_s[at].astype(f32) + matmul_nt(r1_s[at], we1[:width])
    edge_o[at] = grad.astype(bf16)
    a_red.exchange()
    b_red.exchange()
    node_red.gather()
    at = pl.ds(half, edges - half)
    grad = ecot_s[at].astype(f32) + matmul_nt(r1_s[at], we1[:width])
    edge_o[at] = grad.astype(bf16)
    for copy in halos:
        copy.wait()
    spot = lax.broadcasted_iota(jnp.int32, (nodes, slots), 0)
    local = node_o[...]
    for face in range(6):
        values = halo[face * slots : (face + 1) * slots].astype(bf16)
        local = local + matmul(one_hot(spot == faces[face]), values)
    node_o[...] = local
    a_red.gather()
    b_red.gather()
    node_red.wait()
    a_red.wait()
    b_red.wait()


def finish_kernel(
    node, edge, nred, ared, bred, node_o, edge_o, we1_o, weh_o, be_o, ge_o, se_o, wn1_o, wnh_o, bn_o, gn_o
):
    width = node.shape[1]
    node_o[...] = node[...]
    edge_o[...] = edge[...]
    we1_o[...] = ared[: 3 * width]
    weh_o[0] = ared[3 * width : 4 * width]
    weh_o[1] = bred[:width]
    wn1_o[...] = nred[: 2 * width]
    wnh_o[0] = nred[2 * width : 3 * width]
    wnh_o[1] = nred[3 * width : 4 * width]
    be_o[...] = bred[width : width + 3]
    ge_o[...] = bred[width + 3 : width + 4]
    se_o[...] = bred[width + 4 : width + 5]
    bn_o[...] = bred[width + 5 : width + 8]
    gn_o[...] = bred[width + 8 : width + 9]


VMEM = pl.BlockSpec(memory_space=pltpu.VMEM)
HBM = pl.BlockSpec(memory_space=pl.ANY)


def on_device(
    sizes,
    node_latent,
    ghost_latent,
    edge_latent,
    senders,
    receivers,
    export_rows,
    node_cotangent,
    edge_cotangent,
    w_edge_in,
    w_edge_hidden,
    b_edge,
    gain_edge,
    shift_edge,
    w_node_in,
    w_node_hidden,
    b_node,
    gain_node,
):
    f32, bf16 = jnp.float32, jnp.bfloat16
    nodes, width = node_latent.shape[3:]
    slots = ghost_latent.shape[4]
    ghosts = 6 * slots
    edges = edge_latent.shape[3]
    total = nodes + ghosts
    devices = sizes["gx"] * sizes["gy"] * sizes["gz"]
    edge_scale = float(edges * devices) ** (-0.5)
    node_scale = float(nodes * devices) ** (-0.5)

    def padded(rows, group):
        unit = 8 * group_size(group)
        return -(-rows // unit) * unit

    def shape(*dims, dtype=f32):
        return jax.ShapeDtypeStruct(dims, dtype)

    near, far = stage_groups(sizes)
    four, two = padded(4 * width, near), padded(width + 9, far)
    reducers = reducer_scratch(near, far, four, width)
    reducers += reducer_scratch(near, far, four, width)
    reducers += reducer_scratch(far, near, two, width)
    passed = pl.pallas_call(
        functools.partial(block_kernel, sizes, edge_scale, node_scale),
        out_shape=(
            shape(nodes, width),
            shape(edges, width, dtype=bf16),
            shape(four, width),
            shape(four, width),
            shape(two, width),
        ),
        in_specs=[VMEM] * 2 + [HBM] + [VMEM] * 4 + [HBM] + [VMEM] * 9,
        out_specs=(VMEM,) * 5,
        scratch_shapes=[
            pltpu.VMEM((edges, total + nodes), bf16),
            pltpu.VMEM((total + nodes, edges), bf16),
            pltpu.VMEM((total + nodes, width), bf16),
            pltpu.VMEM((edges, width), bf16),
            pltpu.VMEM((edges, width), bf16),
            pltpu.VMEM((edges, width), bf16),
            pltpu.VMEM((edges, width), f32),
            pltpu.VMEM((edges, width), f32),
            pltpu.VMEM((edges, width), f32),
            pltpu.VMEM((edges, width), f32),
            pltpu.VMEM((four, width), f32),
            pltpu.VMEM((four, width), f32),
            pltpu.VMEM((two, width), f32),
            pltpu.VMEM((edges, width), bf16),
            pltpu.VMEM((edges, width), bf16),
            pltpu.VMEM((ghosts, width), f32),
            pltpu.VMEM((ghosts, width), f32),
            pltpu.SemaphoreType.DMA((2,)),
            pltpu.SemaphoreType.DMA((6,)),
            pltpu.SemaphoreType.DMA((6,)),
        ]
        + reducers,
        compiler_params=pltpu.CompilerParams(
            collective_id=0, has_side_effects=True, vmem_limit_bytes=60 * 1024 * 1024
        ),
        name="block_pass",
    )(
        node_latent.reshape(nodes, width),
        ghost_latent.reshape(ghosts, width),
        edge_latent.reshape(edges, width),
        senders.reshape(1, edges),
        receivers.reshape(1, edges),
        export_rows.reshape(6, 1, slots),
        node_cotangent.reshape(nodes, width),
        edge_cotangent.reshape(edges, width),
        w_edge_in,
        w_edge_hidden,
        b_edge,
        gain_edge.reshape(1, width),
        shift_edge.reshape(1, width),
        w_node_in,
        w_node_hidden,
        b_node,
        gain_node.reshape(1, width),
    )

    outs = pl.pallas_call(
        finish_kernel,
        out_shape=(
            shape(nodes, width),
            shape(edges, width, dtype=bf16),
            shape(3 * width, width),
            shape(2, width, width),
            shape(3, width),
            shape(1, width),
            shape(1, width),
            shape(2 * width, width),
            shape(2, width, width),
            shape(3, width),
            shape(1, width),
        ),
        in_specs=[VMEM] * 5,
        out_specs=(VMEM,) * 11,
        name="finish",
    )(*passed)
    node_grad, edge_grad, we1, weh, be, ge, se, wn1, wnh, bn, gn = outs
    return (
        node_grad.reshape(node_latent.shape),
        edge_grad.reshape(edge_latent.shape),
        we1,
        weh,
        be,
        ge.reshape(width),
        se.reshape(width),
        wn1,
        wnh,
        bn,
        gn.reshape(width),
    )


def solution(mesh):
    block = P("gx", "gy", "gz")
    sizes = dict(mesh.shape)
    return jax.shard_map(
        functools.partial(on_device, sizes),
        mesh=mesh,
        in_specs=(block,) * 8 + (P(),) * 9,
        out_specs=(block,) * 2 + (P(),) * 9,
        check_vma=False,
    )
```
